32 devices in a mesh: seq: 8 (over z, y), head: 4 (over x, core).
Axes of the slice: x: 2, y: 2, z: 4, core: 2. Of those that a mesh axis runs over, the one named last changes fastest.
Arguments:
- queries: bfloat16 [4096, 4096], P('seq', 'head'), may hold values from -5 to 5
- keys: bfloat16 [4096, 1024], P('seq', 'head'), may hold values from -5 to 5
- values: bfloat16 [4096, 1024], P('seq', 'head'), may hold values from -5 to 5
- doc_lengths: int32 [16], replicated, may hold values from 1 to 2048, 4096 in all
- out_weight: bfloat16 [4096, 4096], P('head', 'seq'), may hold values from -0.125 to 0.125
Outputs:
- mixed: bfloat16 [4096, 4096], P('seq', 'head')
The draws below stay inside these ranges and needn't reach their ends.
Inputs may be any that keep to these rules, and one draw needn't show every extreme that they name: `doc_lengths`: the lengths sum to 4096, and one document is exactly 2048 tokens long.
All inputs are finite; a program needn't handle non-finite values.
Results may differ from the reference program's by a relative error of at most 0.012.
Values may be sent and summed in bfloat16 or wider, within the bound.
A program may use at most 128 MiB of HBM per device.

```python
import math
import jax
import jax.numpy as jnp
import numpy as np
from jax import lax

D = 4096
HQ = 32
KV = 8
DH = 128
TOK_DEV = 512
TOKENS = 4096
MOST = 2048
DOCS = 16


def draw_keys(key, part):
    base = jnp.clip(jax.random.normal(jax.random.fold_in(key, 1), (TOKENS, KV * DH), jnp.float32), -5.0, 5.0)
    return base.astype(jnp.bfloat16)


def draw_queries(key, part):
    base = jnp.clip(jax.random.normal(jax.random.fold_in(key, 2), (TOKENS, HQ * DH), jnp.float32), -5.0, 5.0)
    return base.astype(jnp.bfloat16)


def raised(array, key, source, target, parts, factor):
    def block_of(axis_at):
        return (jnp.arange(array.shape[axis_at]) // (array.shape[axis_at] // parts)).reshape((-1,) + (1,) * (array.ndim - 1 - axis_at))

    one_side = jax.random.permutation(key, parts)[block_of(target)]
    other_side = (block_of(target) + parts // 2) % parts
    return jnp.where((block_of(source) == one_side) | (block_of(source) == other_side), factor * array, array)


def steps_of(key, dims, cuts, low, high):
    gain, own = 1.0, jax.random.fold_in(key, 6)
    for axis_at, parts in cuts:
        heights = jnp.exp(jax.random.uniform(jax.random.fold_in(own, axis_at), (parts,), jnp.float32, low / len(cuts), high / len(cuts)))
        gain = gain * jnp.repeat(heights, dims[axis_at] // parts).reshape([-1 if axis == axis_at else 1 for axis in range(len(dims))])
    return gain


def length_profile(amount, total, most, slope):
    loads = [(1 << 20) // math.isqrt(grade ** slope) + 1 for grade in range(2, amount + 1)]
    rest, given = total - most - (amount - 1), [1] * (amount - 1)
    while rest > 0:
        free = [i for i in range(amount - 1) if given[i] < most]
        mass, left = sum([loads[i] for i in free]), rest
        for i in free:
            addition = min(most - given[i], max(1, left * loads[i] // mass), rest)
            given[i] = given[i] + addition
            rest = rest - addition
    return np.array([most] + given)


def uneven(stream_key, count, total, limit, slope):
    if count == 2:
        one = jax.random.randint(stream_key, (), max(1, total - limit), min(limit, total - 1) + 1)
        return jnp.stack([one, total - one])
    sizes = jnp.asarray(length_profile(count, total, limit, slope), jnp.int32)
    twos = (count - 1) // 2
    source_of, taker = sizes[1:1 + 2 * twos:2], sizes[2:2 + 2 * twos:2]
    margin = jnp.minimum(source_of - 1, limit - taker)
    passed = jax.random.randint(jax.random.fold_in(stream_key, 1), (twos,), 0, 1 << 20) % (margin + 1)
    sizes = sizes.at[1:1 + 2 * twos:2].set(source_of - passed).at[2:2 + 2 * twos:2].set(taker + passed)
    return sizes[jax.random.permutation(jax.random.fold_in(stream_key, 2), count)]


def normal_values(rng, dims, deviation, limit, split=(), kind=jnp.bfloat16):
    array = jax.random.normal(rng, dims, jnp.float32) * deviation
    if len(split) > 0:
        array = steps_of(rng, dims, split, -0.22, 0.18) * array
    return jnp.clip(array, min=-limit, max=limit).astype(kind)


def heavy_noise(stream_key, dims, width, bound, shards, heavy, held_as=jnp.bfloat16):
    entries = width * jax.random.normal(stream_key, dims, jnp.float32)
    if shards:
        entries = entries * steps_of(stream_key, dims, shards, -0.22, 0.18)
    return jnp.clip(raised(entries, jax.random.fold_in(stream_key, 3), *heavy), -bound, bound).astype(held_as)


def setup_inputs(seed: int = 0) -> dict:
    seeds = jax.random.split(jax.random.key(seed), 6)
    return {
        "queries": draw_queries(jax.random.fold_in(seeds[5], 71), 0),
        "keys": draw_keys(jax.random.fold_in(seeds[5], 71), 0),
        "values": normal_values(seeds[2], (TOKENS, KV * DH), 1.0, 5.0, ((0, 8), (1, 4))),
        "doc_lengths": uneven(seeds[3], DOCS, TOKENS, MOST, 2).astype(jnp.int32),
        "out_weight": heavy_noise(seeds[4], (HQ * DH, D), (HQ * DH) ** -0.5, 0.125, ((0, 4), (1, 8)), (0, 1, 8, 2.0)),
    }


def doc_index(positions, starts):
    return jnp.sum((starts[None, :] <= positions[:, None]).astype(jnp.int32), axis=1) - 1


def reference(queries, keys, values, doc_lengths, out_weight):
    starts = (jnp.cumsum(doc_lengths) - doc_lengths).astype(jnp.int32)
    total_rows = queries.shape[0]
    group_size = HQ // KV
    window = MOST + TOK_DEV
    num_blocks = total_rows // TOK_DEV
    temper = DH ** -0.5

    def attend_block(flat_index):
        q_block = flat_index // KV
        kv_head = flat_index % KV
        q_first = (q_block * TOK_DEV).astype(jnp.int32)
        k_first = jnp.clip(q_first - MOST, 0, total_rows - window).astype(jnp.int32)
        q_rows = lax.dynamic_slice(queries, (q_first, (kv_head * group_size * DH).astype(jnp.int32)), (TOK_DEV, group_size * DH))
        q_rows = q_rows.astype(jnp.float32).reshape(TOK_DEV, group_size, DH)
        k_rows = lax.dynamic_slice(keys, (k_first, (kv_head * DH).astype(jnp.int32)), (window, DH)).astype(jnp.float32)
        v_rows = lax.dynamic_slice(values, (k_first, (kv_head * DH).astype(jnp.int32)), (window, DH)).astype(jnp.float32)
        scores = jnp.einsum("qgd,nd->gqn", q_rows, k_rows) * temper
        q_pos = q_first + jnp.arange(TOK_DEV, dtype=jnp.int32)
        k_pos = k_first + jnp.arange(window, dtype=jnp.int32)
        q_doc = doc_index(q_pos, starts)
        k_doc = doc_index(k_pos, starts)
        allowed = (k_doc[None, :] == q_doc[:, None]) & (k_pos[None, :] <= q_pos[:, None])
        scores = jnp.where(allowed[None], scores, jnp.float32(-1e30))
        row_max = jnp.max(scores, axis=-1, keepdims=True)
        probs = jnp.where(allowed[None], jnp.exp(scores - row_max), jnp.float32(0.0))
        row_sum = jnp.sum(probs, axis=-1)
        weights = probs.astype(jnp.bfloat16)
        result = jnp.einsum("gqn,nd->gqd", weights.astype(jnp.float32), v_rows) / row_sum[..., None]
        return jnp.transpose(result, (1, 0, 2)).reshape(TOK_DEV, group_size * DH).astype(jnp.bfloat16)

    blocks = lax.map(attend_block, jnp.arange(num_blocks * KV, dtype=jnp.int32))
    attn = blocks.reshape(num_blocks, KV, TOK_DEV, group_size * DH)
    attn = jnp.transpose(attn, (0, 2, 1, 3)).reshape(total_rows, HQ * DH)
    return jnp.dot(attn, out_weight, preferred_element_type=jnp.float32).astype(jnp.bfloat16)
```

```python
import functools
import math

import jax
import jax.numpy as jnp
from jax import lax
from jax.experimental import pallas as pl
from jax.experimental.pallas import tpu as pltpu
from jax.sharding import PartitionSpec as P

HQ = 32
KV = 8
DH = 128
MOST = 2048
CHUNKS = 4
MESH = pl.DeviceIdType.MESH


def kernel(
    n_seq, lens_ref, q_ref, k_hbm, v_hbm, w_hbm, out_ref,
    kbuf, vbuf, wbuf, bias, vt, mx, sm, acc, attn, peer,
    give1, got1, keep, give2, got2, give3, got3,
    load_sem, kvz_send, kvy_send, kv_recv, wl_send, wl_recv, wr_send, wr_recv,
    at_send, at_recv, s1_send, s1_recv, s2_send, s2_recv, s3_send, s3_recv,
):
    s, h = lax.axis_index("seq"), lax.axis_index("head")
    pairs = n_seq // 2
    p, m = s // 2, lax.rem(s, 2)
    mate = s + 1 - 2 * m
    right = lax.rem(p + 1, pairs) * 2 + m
    left = lax.rem(p + pairs - 1, pairs) * 2 + m
    near = h + 1 - 2 * lax.rem(h, 2)
    far = lax.rem(h + 2, 4)
    rows = q_ref.shape[0]
    depth, wc = w_hbm.shape
    half = depth // 2
    groups = pairs // 4
    group_size = HQ // KV
    n_left = pairs // 2
    n_right = pairs - 1 - n_left
    part = rows * 2 // CHUNKS
    scale = DH ** (-0.5) * math.log2(math.e)

    def copy(src, dst, send, recv, seq, head):
        return pltpu.make_async_remote_copy(
            src_ref=src, dst_ref=dst, send_sem=send, recv_sem=recv,
            device_id={"seq": seq, "head": head}, device_id_type=MESH,
        )

    def kv_copies(src_slot, dst_slot, j, send, target):
        cols = pl.ds(pl.multiple_of(j * DH, DH), DH)
        return [
            copy(buf.at[src_slot, :, cols], buf.at[dst_slot, :, cols],
                 send.at[j, c], kv_recv.at[dst_slot, j, c], target, h)
            for c, buf in enumerate((kbuf, vbuf))
        ]

    def w_copy(block, part_at, step, send, recv, target):
        piece = wbuf.at[block, pl.ds(part_at * half, half)]
        return copy(piece, piece, send.at[step, part_at], recv.at[step, part_at], target, h)

    def left_copy(step, part_at):
        return w_copy(lax.rem(p + step, pairs), part_at, step, wl_send, wl_recv, left)

    def right_copy(step, part_at):
        return w_copy(lax.rem(p - step + pairs, pairs), part_at, step, wr_send, wr_recv, right)

    loads = [
        pltpu.make_async_copy(k_hbm, kbuf.at[0], load_sem.at[0]),
        pltpu.make_async_copy(v_hbm, vbuf.at[0], load_sem.at[1]),
        pltpu.make_async_copy(w_hbm, wbuf.at[p], load_sem.at[2]),
    ]
    for load in loads:
        load.start()

    barrier = pltpu.get_barrier_semaphore()
    for seq, head in ((mate, h), (left, h), (right, h), (s, near), (s, far)):
        pl.semaphore_signal(barrier, inc=1, device_id={"seq": seq, "head": head}, device_id_type=MESH)
    pl.semaphore_wait(barrier, 5)

    loads[0].wait()
    loads[1].wait()
    has_next = s + 2 < n_seq
    for j in range(2):
        @pl.when(has_next)
        def _():
            for c in kv_copies(0, 2, j, kvz_send.at[0], right):
                c.start()

        @pl.when(m == 0)
        def _():
            for c in kv_copies(0, 1, j, kvy_send.at[0], mate):
                c.start()

    loads[2].wait()
    for a in range(2):
        left_copy(0, a).start()

    q_pos = s * rows + lax.broadcasted_iota(jnp.int32, (1, rows), 1)
    start = jnp.int32(0)
    first = jnp.zeros((1, rows), jnp.int32)
    for d in range(1, lens_ref.shape[0]):
        start = start + lens_ref[d - 1]
        first = jnp.where(q_pos >= start, start, first)

    def finish(j):
        def one(g, _):
            i = j * group_size + g
            full = jnp.transpose(acc[i] / sm[i])
            attn[j, :, pl.ds(pl.multiple_of(g * DH, DH), DH)] = full.astype(jnp.bfloat16)
            return 0

        lax.fori_loop(0, group_size, one, 0)
        copy(attn.at[j], peer.at[j], at_send.at[j], at_recv.at[j], mate, h).start()

    def step(i, _):
        k = jnp.maximum(i - 2, 0)
        w = lax.rem(k, 4)
        slot = jnp.where(i < 2, 0, 2 + 2 * (k // 4) - lax.rem(w, 2))
        j = jnp.where(i < 2, i, w // 2)

        @pl.when((i >= 2) & (s >= slot))
        def _():
            for c in kv_copies(slot, slot, j, kvz_send.at[0], right):
                c.wait_recv()

            @pl.when((slot == 2) & has_next)
            def _():
                for c in kv_copies(2, 4, j, kvz_send.at[1], right):
                    c.start()

            @pl.when(slot == 2)
            def _():
                for c in kv_copies(2, 3 - 2 * m, j, kvy_send.at[1], mate):
                    c.start()

            @pl.when((slot == 4) & (m == 1))
            def _():
                for c in kv_copies(4, 3, j, kvy_send.at[2], mate):
                    c.start()

        @pl.when(i == 4)
        def _():
            for a in range(2):
                right_copy(0, a).start()

        for at, a in ((5, 0), (8, 1)):
            @pl.when(i == at)
            def _():
                left_copy(0, a).wait_recv()
                left_copy(1, a).start()

        @pl.when(s >= slot)
        def _():
            cols = pl.ds(pl.multiple_of(j * DH, DH), DH)
            k_pos = (s - slot) * rows + lax.broadcasted_iota(jnp.int32, (rows, rows), 0)
            bias[...] = jnp.where((k_pos >= first) & (k_pos <= q_pos), 0.0, -1e30)
            vt[...] = jnp.transpose(vbuf[slot, :, cols])

            def one(g, _):
                at = j * group_size + g
                q = q_ref[:, pl.ds(pl.multiple_of(at * DH, DH), DH)]
                scores = lax.dot_general(
                    kbuf[slot, :, cols], q, (((1,), (1,)), ((), ())),
                    preferred_element_type=jnp.float32,
                ) * scale + bias[...]
                top = jnp.max(scores, axis=0, keepdims=True)
                old = jnp.where(i < 2, jnp.full_like(top, -1e30), mx[at])
                new = jnp.maximum(old, top)
                probs = jnp.exp2(scores - new)
                fade = jnp.exp2(old - new)
                mx[at] = new
                total = jnp.sum(probs, axis=0, keepdims=True)
                sm[at] = jnp.where(i < 2, total, sm[at] * fade + total)
                mixed = jnp.dot(vt[...], probs.astype(jnp.bfloat16), preferred_element_type=jnp.float32)

                @pl.when(i < 2)
                def _():
                    acc[at] = mixed

                @pl.when(i >= 2)
                def _():
                    acc[at] = acc[at] * fade + mixed

                return 0

            lax.fori_loop(0, group_size, one, 0)

        for at, jj in ((7, 0), (9, 1)):
            @pl.when(i == at)
            def _():
                finish(jj)

        return 0

    lax.fori_loop(0, 10, step, 0)

    for t in range(1, max(n_left, n_right)):
        for a in range(2):
            if t < n_right:
                right_copy(t - 1, a).wait_recv()
                right_copy(t, a).start()
            if 2 <= t < n_left:
                left_copy(t - 1, a).wait_recv()
                left_copy(t, a).start()
    for a in range(2):
        right_copy(n_right - 1, a).wait_recv()
        left_copy(n_left - 1, a).wait_recv()

    def attn_copy(j):
        return copy(attn.at[j], peer.at[j], at_send.at[j], at_recv.at[j], mate, h)

    for j in range(2):
        attn_copy(j).wait_recv()

    def first_copy(r):
        return copy(give1.at[r], got1.at[r], s1_send.at[r], s1_recv.at[r], s, near)

    def second_copy(r):
        return copy(give2.at[r], got2.at[r], s2_send.at[r], s2_recv.at[r], s, far)

    def third_copy(r):
        return copy(give3.at[r], got3.at[r], s3_send.at[r], s3_recv.at[r], mate, h)

    per_side = CHUNKS // 2

    def product(source, at, group, store):
        x0 = source[0, pl.ds(at, part), :]
        x1 = source[1, pl.ds(at, part), :]
        for g in range(groups):
            block = group * groups + g
            store(g, jnp.dot(x0, wbuf[block, :half, :], preferred_element_type=jnp.float32)
                  + jnp.dot(x1, wbuf[block, half:, :], preferred_element_type=jnp.float32))

    def multiply(r, source, at):
        for x in range(2):
            def put(g, y, x=x):
                give1[r, x, :, g * wc:(g + 1) * wc] = y.astype(jnp.bfloat16)

            product(source, at, 2 * x + 1 - lax.rem(h, 2), put)
        first_copy(r).start()
        for x in range(2):
            def hold(g, y, x=x):
                keep[r, x, :, g * wc:(g + 1) * wc] = y

            product(source, at, 2 * x + lax.rem(h, 2), hold)

    mine, other = h // 2, 1 - h // 2

    def second(r):
        first_copy(r).wait_recv()
        give2[r] = (keep[r, other] + got1[r, other].astype(jnp.float32)).astype(jnp.bfloat16)
        second_copy(r).start()

    def result(r):
        second_copy(r).wait_recv()
        full = keep[r, mine] + got1[r, mine].astype(jnp.float32) + got2[r].astype(jnp.float32)
        return full.astype(jnp.bfloat16)

    def place(at, member, value):
        for mm in range(2):
            @pl.when(member == mm)
            def _():
                for g in range(groups):
                    c = (2 * g + mm) * wc
                    out_ref[pl.ds(at, part), c:c + wc] = value[:, g * wc:(g + 1) * wc]

    def round_trip(r, _):
        @pl.when(r < per_side)
        def _():
            multiply(r, peer, pl.multiple_of(r * part, part))

        @pl.when((r >= per_side) & (r < CHUNKS))
        def _():
            multiply(r, attn, pl.multiple_of((r - per_side) * part, part))

        @pl.when(r >= 1)
        def _():
            second(r - 1)

        return 0

    lax.fori_loop(0, CHUNKS + 1, round_trip, 0)

    for r in range(per_side):
        give3[r] = result(r)
        third_copy(r).start()
    for r in range(per_side, CHUNKS):
        place((r - per_side) * part, m, result(r))
    for r in range(per_side):
        third_copy(r).wait_recv()
        place(r * part, 1 - m, got3[r])

    for j in range(2):
        @pl.when(has_next)
        def _():
            for c in kv_copies(0, 2, j, kvz_send.at[0], right):
                c.wait_send()

        @pl.when((s >= 2) & has_next)
        def _():
            for c in kv_copies(2, 4, j, kvz_send.at[1], right):
                c.wait_send()

        @pl.when(m == 0)
        def _():
            for c in kv_copies(0, 1, j, kvy_send.at[0], mate):
                c.wait_send()

        @pl.when(s >= 2)
        def _():
            for c in kv_copies(2, 3 - 2 * m, j, kvy_send.at[1], mate):
                c.wait_send()

        @pl.when((s >= 4) & (m == 1))
        def _():
            for c in kv_copies(4, 3, j, kvy_send.at[2], mate):
                c.wait_send()

        attn_copy(j).wait_send()
        for t in range(n_left):
            left_copy(t, j).wait_send()
        for t in range(n_right):
            right_copy(t, j).wait_send()
    for r in range(CHUNKS):
        first_copy(r).wait_send()
        second_copy(r).wait_send()
    for r in range(per_side):
        third_copy(r).wait_send()


def body(n_seq, queries, keys, values, doc_lengths, out_weight):
    rows, width = queries.shape
    kv_width = keys.shape[1]
    depth, wc = out_weight.shape
    pairs = n_seq // 2
    n_left = pairs // 2
    n_right = pairs - 1 - n_left
    heads = width // DH
    part = rows * 2 // CHUNKS
    cw = pairs // 4 * wc
    slots = -(-(MOST - 1) // rows) + 1
    vmem = pl.BlockSpec(memory_space=pltpu.VMEM)
    hbm = pl.BlockSpec(memory_space=pl.ANY)
    bf, f32, dma = jnp.bfloat16, jnp.float32, pltpu.SemaphoreType.DMA
    return pl.pallas_call(
        functools.partial(kernel, n_seq),
        out_shape=jax.ShapeDtypeStruct((rows, wc * 2 * (pairs // 4)), bf),
        in_specs=[pl.BlockSpec(memory_space=pltpu.SMEM), vmem, hbm, hbm, hbm],
        out_specs=vmem,
        scratch_shapes=[
            pltpu.VMEM((slots, rows, kv_width), bf),
            pltpu.VMEM((slots, rows, kv_width), bf),
            pltpu.VMEM((pairs, depth, wc), bf),
            pltpu.VMEM((rows, rows), f32),
            pltpu.VMEM((DH, rows), bf),
            pltpu.VMEM((heads, 1, rows), f32),
            pltpu.VMEM((heads, 1, rows), f32),
            pltpu.VMEM((heads, DH, rows), f32),
            pltpu.VMEM((2, rows, width // 2), bf),
            pltpu.VMEM((2, rows, width // 2), bf),
            pltpu.VMEM((CHUNKS, 2, part, cw), bf),
            pltpu.VMEM((CHUNKS, 2, part, cw), bf),
            pltpu.VMEM((CHUNKS, 2, part, cw), f32),
            pltpu.VMEM((CHUNKS, part, cw), bf),
            pltpu.VMEM((CHUNKS, part, cw), bf),
            pltpu.VMEM((CHUNKS // 2, part, cw), bf),
            pltpu.VMEM((CHUNKS // 2, part, cw), bf),
            dma((3,)), dma((2, 2, 2)), dma((3, 2, 2)), dma((slots, 2, 2)),
            dma((n_left, 2)), dma((n_left, 2)), dma((n_right, 2)), dma((n_right, 2)),
            dma((2,)), dma((2,)), dma((CHUNKS,)), dma((CHUNKS,)),
            dma((CHUNKS,)), dma((CHUNKS,)), dma((CHUNKS // 2,)), dma((CHUNKS // 2,)),
        ],
        compiler_params=pltpu.CompilerParams(
            collective_id=0, has_side_effects=True, vmem_limit_bytes=56 * 1024 * 1024
        ),
    )(doc_lengths, queries, keys, values, out_weight)


def solution(mesh):
    return jax.shard_map(
        functools.partial(body, mesh.shape["seq"]),
        mesh=mesh,
        in_specs=(P("seq", "head"), P("seq", "head"), P("seq", "head"), P(), P("head", "seq")),
        out_specs=P("seq", "head"),
        check_vma=False,
    )
```

```python
import functools
import math

import jax
import jax.numpy as jnp
from jax import lax
from jax.experimental import pallas as pl
from jax.experimental.pallas import tpu as pltpu
from jax.sharding import PartitionSpec as P

HQ = 32
KV = 8
DH = 128
MOST = 2048
CHUNKS = 4
MESH = pl.DeviceIdType.MESH


def kernel(
    n_seq, lens_ref, q_ref, k_hbm, v_hbm, w_hbm, out_ref,
    kbuf, vbuf, wbuf, bias, vt, mx, sm, acc, both,
    tmp, keep, sum1, sum2, give3, got3,
    load_sem, kvz_send, kvy_send, kv_recv, wl_send, wl_recv, wr_send, wr_recv,
    at_send, at_recv, s1_send, s1_recv, s2_send, s2_recv, s3_send, s3_recv,
):
    s, h = lax.axis_index("seq"), lax.axis_index("head")
    pairs = n_seq // 2
    p, m = s // 2, lax.rem(s, 2)
    mate = s + 1 - 2 * m
    right = lax.rem(p + 1, pairs) * 2 + m
    left = lax.rem(p + pairs - 1, pairs) * 2 + m
    near = h + 1 - 2 * lax.rem(h, 2)
    far = lax.rem(h + 2, 4)
    rows = q_ref.shape[0]
    depth, wc = w_hbm.shape
    half = depth // 2
    groups = pairs // 4
    group_size = HQ // KV
    part = rows * 2 // CHUNKS
    has_up, has_down = p + 1 < pairs, p >= 1
    scale = DH ** (-0.5) * math.log2(math.e)

    def copy(src, dst, send, recv, seq, head):
        return pltpu.make_async_remote_copy(
            src_ref=src, dst_ref=dst, send_sem=send, recv_sem=recv,
            device_id={"seq": seq, "head": head}, device_id_type=MESH,
        )

    def kv_copies(src_slot, dst_slot, j, send, target):
        cols = pl.ds(pl.multiple_of(j * DH, DH), DH)
        return [
            copy(buf.at[src_slot, :, cols], buf.at[dst_slot, :, cols],
                 send.at[j, c], kv_recv.at[dst_slot, j, c], target, h)
            for c, buf in enumerate((kbuf, vbuf))
        ]

    def w_copy(block, part_at, step, send, recv, target):
        piece = wbuf.at[block, pl.ds(part_at * half, half)]
        return copy(piece, piece, send.at[step, part_at], recv.at[step, part_at], target, h)

    def left_copy(step, part_at):
        return w_copy(jnp.minimum(p + step, pairs - 1), part_at, step, wl_send, wl_recv, left)

    def right_copy(step, part_at):
        return w_copy(jnp.maximum(p - step, 0), part_at, step, wr_send, wr_recv, right)

    loads = [
        pltpu.make_async_copy(k_hbm, kbuf.at[0], load_sem.at[0]),
        pltpu.make_async_copy(v_hbm, vbuf.at[0], load_sem.at[1]),
        pltpu.make_async_copy(w_hbm, wbuf.at[p], load_sem.at[2]),
    ]
    for load in loads:
        load.start()

    barrier = pltpu.get_barrier_semaphore()
    for seq, head in ((mate, h), (left, h), (right, h), (s, near), (s, far)):
        pl.semaphore_signal(barrier, inc=1, device_id={"seq": seq, "head": head}, device_id_type=MESH)
    pl.semaphore_wait(barrier, 5)

    loads[0].wait()
    loads[1].wait()
    has_next = s + 2 < n_seq
    for j in range(2):
        @pl.when(has_next)
        def _():
            for c in kv_copies(0, 2, j, kvz_send.at[0], right):
                c.start()

        @pl.when(m == 0)
        def _():
            for c in kv_copies(0, 1, j, kvy_send.at[0], mate):
                c.start()

    loads[2].wait()

    @pl.when(has_down)
    def _():
        for a in range(2):
            left_copy(0, a).start()

    q_pos = s * rows + lax.broadcasted_iota(jnp.int32, (1, rows), 1)
    start = jnp.int32(0)
    first = jnp.zeros((1, rows), jnp.int32)
    for d in range(1, lens_ref.shape[0]):
        start = start + lens_ref[d - 1]
        first = jnp.where(q_pos >= start, start, first)

    def attn_copy(j):
        return copy(both.at[1, j], both.at[0, j], at_send.at[j], at_recv.at[j], mate, h)

    def finish(j):
        def one(g, _):
            i = j * group_size + g
            full = jnp.transpose(acc[i] / sm[i])
            both[1, j, :, pl.ds(pl.multiple_of(g * DH, DH), DH)] = full.astype(jnp.bfloat16)
            return 0

        lax.fori_loop(0, group_size, one, 0)
        attn_copy(j).start()

    def step(i, _):
        k = jnp.maximum(i - 2, 0)
        w = lax.rem(k, 4)
        slot = jnp.where(i < 2, 0, 2 + 2 * (k // 4) - lax.rem(w, 2))
        j = jnp.where(i < 2, i, w // 2)

        @pl.when((i >= 2) & (s >= slot))
        def _():
            for c in kv_copies(slot, slot, j, kvz_send.at[0], right):
                c.wait_recv()

            @pl.when((slot == 2) & has_next)
            def _():
                for c in kv_copies(2, 4, j, kvz_send.at[1], right):
                    c.start()

            @pl.when(slot == 2)
            def _():
                for c in kv_copies(2, 3 - 2 * m, j, kvy_send.at[1], mate):
                    c.start()

            @pl.when((slot == 4) & (m == 1))
            def _():
                for c in kv_copies(4, 3, j, kvy_send.at[2], mate):
                    c.start()

        @pl.when((i == 4) & has_up)
        def _():
            for a in range(2):
                right_copy(0, a).start()

        for at, a in ((5, 0), (8, 1)):
            @pl.when((i == at) & has_up)
            def _():
                left_copy(0, a).wait_recv()

                @pl.when(has_down)
                def _():
                    left_copy(1, a).start()

        @pl.when(s >= slot)
        def _():
            cols = pl.ds(pl.multiple_of(j * DH, DH), DH)
            k_pos = (s - slot) * rows + lax.broadcasted_iota(jnp.int32, (rows, rows), 0)
            bias[...] = jnp.where((k_pos >= first) & (k_pos <= q_pos), 0.0, -1e30)
            vt[...] = jnp.transpose(vbuf[slot, :, cols])

            def one(g, _):
                at = j * group_size + g
                q = q_ref[:, pl.ds(pl.multiple_of(at * DH, DH), DH)]
                scores = lax.dot_general(
                    kbuf[slot, :, cols], q, (((1,), (1,)), ((), ())),
                    preferred_element_type=jnp.float32,
                ) * scale + bias[...]
                top = jnp.max(scores, axis=0, keepdims=True)
                old = jnp.where(i < 2, jnp.full_like(top, -1e30), mx[at])
                new = jnp.maximum(old, top)
                probs = jnp.exp2(scores - new)
                fade = jnp.exp2(old - new)
                mx[at] = new
                total = jnp.sum(probs, axis=0, keepdims=True)
                sm[at] = jnp.where(i < 2, total, sm[at] * fade + total)
                mixed = jnp.dot(vt[...], probs.astype(jnp.bfloat16), preferred_element_type=jnp.float32)

                @pl.when(i < 2)
                def _():
                    acc[at] = mixed

                @pl.when(i >= 2)
                def _():
                    acc[at] = acc[at] * fade + mixed

                return 0

            lax.fori_loop(0, group_size, one, 0)

        for at, jj in ((7, 0), (9, 1)):
            @pl.when(i == at)
            def _():
                finish(jj)

        return 0

    lax.fori_loop(0, 10, step, 0)

    for j in range(2):
        attn_copy(j).wait_recv()

    per_side = CHUNKS // 2

    def first_copy(b, r):
        return copy(sum1.at[b, r], sum1.at[b, r], s1_send.at[b, r], s1_recv.at[b, r], s, near)

    def second_copy(b, r):
        return copy(sum2.at[b, r], sum2.at[b, r], s2_send.at[b, r], s2_recv.at[b, r], s, far)

    def third_copy(g, r):
        return copy(give3.at[g, r], got3.at[g, r], s3_send.at[g, r], s3_recv.at[g, r], mate, h)

    def odd(b):
        return lax.rem(b // groups + h, 2) == 1

    def block_step(e, _):
        d = (e + 1) // 2
        from_up = lax.rem(e, 2) == 1
        b = jnp.where(from_up, p + d, p - d)
        exists = (b >= 0) & (b < pairs)
        b = jnp.clip(b, 0, pairs - 1)

        @pl.when(exists & (e >= 2))
        def _():
            for a in range(2):
                @pl.when(from_up)
                def _():
                    left_copy(d - 1, a).wait_recv()

                    @pl.when(has_down)
                    def _():
                        left_copy(d, a).start()

                @pl.when(jnp.logical_not(from_up))
                def _():
                    right_copy(d - 1, a).wait_recv()

                    @pl.when(has_up)
                    def _():
                        right_copy(d, a).start()

        @pl.when(exists)
        def _():
            away = odd(b)

            def chunk(r, _):
                side = r // per_side
                at = pl.multiple_of(lax.rem(r, per_side) * part, part)
                y = (jnp.dot(both[side, 0, pl.ds(at, part), :], wbuf[b, :half, :],
                             preferred_element_type=jnp.float32)
                     + jnp.dot(both[side, 1, pl.ds(at, part), :], wbuf[b, half:, :],
                               preferred_element_type=jnp.float32))

                @pl.when(away)
                def _():
                    sum1[b, r] = y.astype(jnp.bfloat16)
                    first_copy(b, r).start()

                @pl.when(jnp.logical_not(away))
                def _():
                    tmp[r] = y

                return 0

            lax.fori_loop(0, CHUNKS, chunk, 0)

            @pl.when(jnp.logical_not(away))
            def _():
                home = b // groups == h
                g = lax.rem(b, groups)

                def settle(r, _):
                    first_copy(b, r).wait_recv()
                    y = tmp[r] + sum1[b, r].astype(jnp.float32)

                    @pl.when(home)
                    def _():
                        keep[g, r] = y

                    @pl.when(jnp.logical_not(home))
                    def _():
                        sum2[b, r] = y.astype(jnp.bfloat16)
                        second_copy(b, r).start()

                    return 0

                lax.fori_loop(0, CHUNKS, settle, 0)

        return 0

    lax.fori_loop(0, 2 * pairs - 1, block_step, 0)

    def result(g, r):
        b = h * groups + g
        second_copy(b, r).wait_recv()
        return (keep[g, r] + sum2[b, r].astype(jnp.float32)).astype(jnp.bfloat16)

    def place(g, at, member, value):
        for mm in range(2):
            @pl.when(member == mm)
            def _():
                c = (2 * g + mm) * wc
                out_ref[at:at + part, c:c + wc] = value

    for g in range(groups):
        for r in range(per_side):
            give3[g, r] = result(g, r)
            third_copy(g, r).start()
    for g in range(groups):
        for r in range(per_side, CHUNKS):
            place(g, (r - per_side) * part, m, result(g, r))
    for g in range(groups):
        for r in range(per_side):
            third_copy(g, r).wait_recv()
            place(g, r * part, 1 - m, got3[g, r])

    for j in range(2):
        @pl.when(has_next)
        def _():
            for c in kv_copies(0, 2, j, kvz_send.at[0], right):
                c.wait_send()

        @pl.when((s >= 2) & has_next)
        def _():
            for c in kv_copies(2, 4, j, kvz_send.at[1], right):
                c.wait_send()

        @pl.when(m == 0)
        def _():
            for c in kv_copies(0, 1, j, kvy_send.at[0], mate):
                c.wait_send()

        @pl.when(s >= 2)
        def _():
            for c in kv_copies(2, 3 - 2 * m, j, kvy_send.at[1], mate):
                c.wait_send()

        @pl.when((s >= 4) & (m == 1))
        def _():
            for c in kv_copies(4, 3, j, kvy_send.at[2], mate):
                c.wait_send()

        attn_copy(j).wait_send()
        for t in range(pairs - 1):
            @pl.when(has_down & (p + t < pairs))
            def _():
                left_copy(t, j).wait_send()

            @pl.when(has_up & (p - t >= 0))
            def _():
                right_copy(t, j).wait_send()

    def drain(b, _):
        for r in range(CHUNKS):
            @pl.when(odd(b))
            def _():
                first_copy(b, r).wait_send()

            @pl.when(jnp.logical_not(odd(b)) & (b // groups != h))
            def _():
                second_copy(b, r).wait_send()

        return 0

    lax.fori_loop(0, pairs, drain, 0)
    for g in range(groups):
        for r in range(per_side):
            third_copy(g, r).wait_send()


def body(n_seq, queries, keys, values, doc_lengths, out_weight):
    rows, width = queries.shape
    kv_width = keys.shape[1]
    depth, wc = out_weight.shape
    pairs = n_seq // 2
    groups = pairs // 4
    heads = width // DH
    part = rows * 2 // CHUNKS
    slots = -(-(MOST - 1) // rows) + 1
    vmem = pl.BlockSpec(memory_space=pltpu.VMEM)
    hbm = pl.BlockSpec(memory_space=pl.ANY)
    bf, f32, dma = jnp.bfloat16, jnp.float32, pltpu.SemaphoreType.DMA
    return pl.pallas_call(
        functools.partial(kernel, n_seq),
        out_shape=jax.ShapeDtypeStruct((rows, wc * 2 * (pairs // 4)), bf),
        in_specs=[pl.BlockSpec(memory_space=pltpu.SMEM), vmem, hbm, hbm, hbm],
        out_specs=vmem,
        scratch_shapes=[
            pltpu.VMEM((slots, rows, kv_width), bf),
            pltpu.VMEM((slots, rows, kv_width), bf),
            pltpu.VMEM((pairs, depth, wc), bf),
            pltpu.VMEM((rows, rows), f32),
            pltpu.VMEM((DH, rows), bf),
            pltpu.VMEM((heads, 1, rows), f32),
            pltpu.VMEM((heads, 1, rows), f32),
            pltpu.VMEM((heads, DH, rows), f32),
            pltpu.VMEM((2, 2, rows, width // 2), bf),
            pltpu.VMEM((CHUNKS, part, wc), f32),
            pltpu.VMEM((groups, CHUNKS, part, wc), f32),
            pltpu.VMEM((pairs, CHUNKS, part, wc), bf),
            pltpu.VMEM((pairs, CHUNKS, part, wc), bf),
            pltpu.VMEM((groups, CHUNKS // 2, part, wc), bf),
            pltpu.VMEM((groups, CHUNKS // 2, part, wc), bf),
            dma((3,)), dma((2, 2, 2)), dma((3, 2, 2)), dma((slots, 2, 2)),
            dma((pairs, 2)), dma((pairs, 2)), dma((pairs, 2)), dma((pairs, 2)),
            dma((2,)), dma((2,)), dma((pairs, CHUNKS)), dma((pairs, CHUNKS)),
            dma((pairs, CHUNKS)), dma((pairs, CHUNKS)),
            dma((groups, CHUNKS // 2)), dma((groups, CHUNKS // 2)),
        ],
        compiler_params=pltpu.CompilerParams(
            collective_id=0, has_side_effects=True, vmem_limit_bytes=56 * 1024 * 1024
        ),
    )(doc_lengths, queries, keys, values, out_weight)


def solution(mesh):
    return jax.shard_map(
        functools.partial(body, mesh.shape["seq"]),
        mesh=mesh,
        in_specs=(P("seq", "head"), P("seq", "head"), P("seq", "head"), P(), P("head", "seq")),
        out_specs=P("seq", "head"),
        check_vma=False,
    )
```
